32 devices in a mesh: tube: 4 (over z), lon: 8 (over y, x, core).
Axes of the slice: x: 2, y: 2, z: 4, core: 2. Of those that a mesh axis runs over, the one named last changes fastest.
Arguments:
- density: float32 [7, 128, 64, 128], P(None, 'tube', 'lon'), may hold values from 0.5 to 5
- pedersen: float32 [128, 64, 128], P('tube', 'lon'), may hold values from 0.1 to 10
- neutral_wind: float32 [128, 64, 128], P('tube', 'lon'), may hold values from -6 to 6
- along_courant: float32 [7, 128], P(None, 'tube'), may hold values from 0.45 to 20000
Outputs:
- density_next: float32 [7, 128, 64, 128], P(None, 'tube', 'lon')
- potential: float32 [64, 128], P('lon')
The draws below stay inside these ranges and needn't reach their ends.
All inputs are finite; a program needn't handle non-finite values.
Results may differ from the reference program's by a relative error of at most 0.00016.
Values sent between devices are 32-bit elements; how exact they have to be, the bound alone decides.
No kernel may reach another device: no remote copies, remote signals or barrier semaphores. Data moves between devices by JAX's collectives and lax.ppermute only.
A program may use at most 64 MiB of HBM per device.

```python
import math
import jax
import jax.numpy as jnp
from jax import lax

ION_SPECIES = 7
LAT = 128
LEVELS = 3
CYCLES = 3
LINE_POINTS = 128
LON = 64


def draw_along_courant(key, part):
    first, second, third_part = jax.random.split(jax.random.fold_in(key, 17), 3)
    base = jax.random.uniform(first, (ION_SPECIES, 1), jnp.float32, 0.0, 9.9)
    rough = 0.5 * jax.random.normal(second, (ION_SPECIES, LINE_POINTS), jnp.float32)
    logarithm_rate = jnp.clip(base + rough, -0.7, 9.9)
    source_pulses = jax.random.randint(third_part, (ION_SPECIES, LINE_POINTS), 0, LINE_POINTS) < 3
    return jnp.where(source_pulses, 1.0, jnp.exp(logarithm_rate)).astype(jnp.float32)


def draw_pedersen(key, part):
    lon_key, lat_key, rough_key = jax.random.split(jax.random.fold_in(key, 29), 3)
    lon_levels = jax.random.uniform(lon_key, (16,), jnp.float32, -1.6, 1.6)
    lat_levels = jax.random.uniform(lat_key, (8,), jnp.float32, -1.6, 1.6)
    lon_block = (jnp.arange(LON) * 16 // LON).astype(jnp.int32)
    lat_block = (jnp.arange(LAT) * 8 // LAT).astype(jnp.int32)
    level = lon_levels[lon_block][:, None] + lat_levels[lat_block][None, :]
    rough = jnp.clip(0.35 * jax.random.normal(rough_key, (LINE_POINTS, LON, LAT), jnp.float32), -0.7, 0.7)
    return jnp.clip(jnp.exp(level[None, :, :] + rough), 0.1, 10.0).astype(jnp.float32)


def levels(rng, shape, pieces, least, largest):
    level, own = 1.0, jax.random.fold_in(rng, 6)
    for axis_at, blocks in pieces:
        draws = jnp.exp(jax.random.uniform(jax.random.fold_in(own, axis_at), (blocks,), jnp.float32, least / len(pieces), largest / len(pieces)))
        level = level * jnp.repeat(draws, shape[axis_at] // blocks).reshape([-1 if axis == axis_at else 1 for axis in range(len(shape))])
    return level


def scatter_about(rng, dims, width, reach, cuts=(), held_as=jnp.bfloat16):
    loudness = levels(rng, dims, cuts, -0.22, 0.18) if cuts else 1.0
    drawn = jax.random.normal(rng, dims, jnp.float32) * width * loudness
    return jnp.minimum(jnp.maximum(drawn, -reach), reach).astype(held_as)


def setup_inputs(seed: int = 0) -> dict:
    key_list = jax.random.split(jax.random.key(seed), 5)
    density = jnp.clip(jnp.exp(math.log(5.0) - 2.3025851 * jax.random.uniform(key_list[0], (ION_SPECIES, LINE_POINTS, LON, LAT), jnp.float32) ** levels(key_list[0], (ION_SPECIES, LINE_POINTS, LON, LAT), ((1, 4), (2, 8)), -0.2, 0.2)), 0.5, 5.0)
    pedersen = draw_pedersen(jax.random.fold_in(key_list[4], 71), 0)
    neutral_wind = scatter_about(key_list[2], (LINE_POINTS, LON, LAT), 1.0, 6.0, ((0, 4), (1, 8)), jnp.float32)
    along_courant = draw_along_courant(jax.random.fold_in(key_list[4], 71), 0)
    return {"density": density, "pedersen": pedersen, "neutral_wind": neutral_wind, "along_courant": along_courant}


SCREENING = 0.005
RELAXATION = 0.8
DRIFT_GAIN = 1.0
COURANT_CAP = 0.2

def lat_zeros(periodic_copy):
    return jnp.pad(periodic_copy, ((0, 0), (1, 1)))

def grid_pad(grid_field):
    periodic_copy = jnp.concatenate([grid_field[-1:], grid_field, grid_field[:1]], axis=0)
    return lat_zeros(periodic_copy)

def face_weights(cond_pad):
    middle = cond_pad[1:-1, 1:-1]
    return (0.5 * (cond_pad[:-2, 1:-1] + middle), 0.5 * (cond_pad[2:, 1:-1] + middle), 0.5 * (cond_pad[1:-1, :-2] + middle), 0.5 * (cond_pad[1:-1, 2:] + middle))

def apply_operator(field_pad, weights, level_scale):
    middle = field_pad[1:-1, 1:-1]
    net_flux = weights[0] * (middle - field_pad[:-2, 1:-1]) + weights[1] * (middle - field_pad[2:, 1:-1])
    net_flux = net_flux + weights[2] * (middle - field_pad[1:-1, :-2]) + weights[3] * (middle - field_pad[1:-1, 2:])
    return level_scale * net_flux + SCREENING * middle

def diagonal_of(weights, level_scale):
    return level_scale * (weights[0] + weights[1] + weights[2] + weights[3]) + SCREENING

def coarsen(grid_field):
    return 0.25 * grid_field.reshape(grid_field.shape[0] // 2, 2, grid_field.shape[1] // 2, 2).sum(axis=(1, 3))

def refine(grid_field):
    return jnp.repeat(jnp.repeat(grid_field, 2, axis=0), 2, axis=1)

def dense_operator(grid_cond, level_scale):
    unknowns = grid_cond.shape[0] * grid_cond.shape[1]
    weights = face_weights(grid_pad(grid_cond))
    unit_fields = jnp.eye(unknowns, dtype=jnp.float32).reshape(unknowns, grid_cond.shape[0], grid_cond.shape[1])
    matrix_rows = jax.vmap(lambda unit_field: apply_operator(grid_pad(unit_field), weights, level_scale))(unit_fields)
    return matrix_rows.reshape(unknowns, unknowns)

def vcycle(level_index, right_side, start_field, weights, diagonals, padder, coarse_solve):
    if level_index == len(weights):
        return coarse_solve(right_side)
    level_scale = 0.25 ** level_index
    if start_field is None:
        relaxed_potential = RELAXATION * right_side / diagonals[level_index]
    else:
        relaxed_potential = start_field + RELAXATION * (right_side - apply_operator(padder(start_field), weights[level_index], level_scale)) / diagonals[level_index]
    residual = right_side - apply_operator(padder(relaxed_potential), weights[level_index], level_scale)
    relaxed_potential = relaxed_potential + refine(vcycle(level_index + 1, coarsen(residual), None, weights, diagonals, padder, coarse_solve))
    return relaxed_potential + RELAXATION * (right_side - apply_operator(padder(relaxed_potential), weights[level_index], level_scale)) / diagonals[level_index]

def drifts(padded):
    lon_drift = COURANT_CAP * jnp.tanh(-DRIFT_GAIN * 0.25 * (padded[:-1, 2:] + padded[1:, 2:] - (padded[:-1, :-2] + padded[1:, :-2])))
    lat_raw = DRIFT_GAIN * 0.25 * (padded[2:, :-1] + padded[2:, 1:] - (padded[:-2, :-1] + padded[:-2, 1:]))
    column = jnp.arange(lat_raw.shape[1])
    inside = (column > 0) & (column < lat_raw.shape[1] - 1)
    lat_drift = jnp.where(inside[None, :], COURANT_CAP * jnp.tanh(lat_raw), 0.0)
    return (lon_drift, lat_drift)

def transport(rimmed, lon_drift, lat_drift):
    interior = rimmed[:, :, 1:-1]
    east_flux = jnp.maximum(lon_drift, 0.0) * rimmed[:, :, :-1] + jnp.minimum(lon_drift, 0.0) * rimmed[:, :, 1:]
    lat_padded = jnp.pad(interior, ((0, 0), (0, 0), (0, 0), (1, 1)))
    north_flux = jnp.maximum(lat_drift, 0.0) * lat_padded[..., :-1] + jnp.minimum(lat_drift, 0.0) * lat_padded[..., 1:]
    return interior - (east_flux[:, :, 1:] - east_flux[:, :, :-1]) - (north_flux[..., 1:] - north_flux[..., :-1])

def reference(density, pedersen, neutral_wind, along_courant):
    conductance = jnp.sum(pedersen, axis=0) / LINE_POINTS
    source = jnp.sum(pedersen * neutral_wind, axis=0) / LINE_POINTS
    conductances = [conductance]
    for level_index in range(LEVELS):
        conductances.append(coarsen(conductances[-1]))
    weights = [face_weights(grid_pad(conductances[level_index])) for level_index in range(LEVELS)]
    diagonals = [diagonal_of(weights[level_index], 0.25 ** level_index) for level_index in range(LEVELS)]
    factor = jnp.linalg.cholesky(dense_operator(conductances[LEVELS], 0.25 ** LEVELS))

    def coarse_solve(right_side):
        return jax.scipy.linalg.cho_solve((factor, True), right_side.reshape(-1)).reshape(right_side.shape)
    potential = None
    for sweep_index in range(CYCLES):
        potential = vcycle(0, source, potential, weights, diagonals, grid_pad, coarse_solve)
    keep_rate = along_courant / (1.0 + along_courant)
    inflow = density / (1.0 + along_courant)[:, :, None, None]

    def advance(carried, inputs_now):
        retain, arriving = inputs_now
        carried = retain[:, None, None] * carried + arriving
        return (carried, carried)
    initial = jnp.zeros((density.shape[0], density.shape[2], density.shape[3]), jnp.float32)
    _, aligned = lax.scan(advance, initial, (jnp.moveaxis(keep_rate, 1, 0), jnp.moveaxis(inflow, 1, 0)))
    aligned = jnp.moveaxis(aligned, 0, 1)
    rimmed = jnp.concatenate([aligned[:, :, -1:], aligned, aligned[:, :, :1]], axis=2)
    lon_drift, lat_drift = drifts(grid_pad(potential))
    return (transport(rimmed, lon_drift, lat_drift), potential)
```

```python
import functools

import jax
import jax.numpy as jnp
from jax import lax
from jax.experimental import pallas as pl
from jax.experimental.pallas import tpu as pltpu
from jax.sharding import PartitionSpec as P

LEVELS = 3
CYCLES = 3


SCREENING = 0.005
RELAXATION = 0.8
DRIFT_GAIN = 1.0
COURANT_CAP = 0.2
ALL_AXES = ("tube", "lon")


def lat_zeros(periodic_copy):
    return jnp.pad(periodic_copy, ((0, 0), (1, 1)))


def grid_pad(grid_field):
    periodic_copy = jnp.concatenate([grid_field[-1:], grid_field, grid_field[:1]], axis=0)
    return lat_zeros(periodic_copy)


def face_weights(cond_pad):
    middle = cond_pad[1:-1, 1:-1]
    return (
        0.5 * (cond_pad[:-2, 1:-1] + middle),
        0.5 * (cond_pad[2:, 1:-1] + middle),
        0.5 * (cond_pad[1:-1, :-2] + middle),
        0.5 * (cond_pad[1:-1, 2:] + middle),
    )


def apply_operator(field_pad, weights, level_scale):
    middle = field_pad[1:-1, 1:-1]
    net_flux = weights[0] * (middle - field_pad[:-2, 1:-1]) + weights[1] * (
        middle - field_pad[2:, 1:-1]
    )
    net_flux = (
        net_flux
        + weights[2] * (middle - field_pad[1:-1, :-2])
        + weights[3] * (middle - field_pad[1:-1, 2:])
    )
    return level_scale * net_flux + SCREENING * middle


def diagonal_of(weights, level_scale):
    return level_scale * (weights[0] + weights[1] + weights[2] + weights[3]) + SCREENING


def coarsen(grid_field):
    return 0.25 * grid_field.reshape(grid_field.shape[0] // 2, 2, grid_field.shape[1] // 2, 2).sum(
        axis=(1, 3)
    )


def refine(grid_field):
    return jnp.repeat(jnp.repeat(grid_field, 2, axis=0), 2, axis=1)


def dense_operator(grid_cond, level_scale):
    unknowns = grid_cond.shape[0] * grid_cond.shape[1]
    weights = face_weights(grid_pad(grid_cond))
    unit_fields = jnp.eye(unknowns, dtype=jnp.float32).reshape(
        unknowns, grid_cond.shape[0], grid_cond.shape[1]
    )
    matrix_rows = jax.vmap(
        lambda unit_field: apply_operator(grid_pad(unit_field), weights, level_scale)
    )(unit_fields)
    return matrix_rows.reshape(unknowns, unknowns)


def vcycle(level_index, right_side, start_field, weights, diagonals, padder, coarse_solve):
    if level_index == len(weights):
        return coarse_solve(right_side)
    level_scale = 0.25**level_index
    if start_field is None:
        relaxed_potential = RELAXATION * right_side / diagonals[level_index]
    else:
        relaxed_potential = (
            start_field
            + RELAXATION
            * (right_side - apply_operator(padder(start_field), weights[level_index], level_scale))
            / diagonals[level_index]
        )
    residual = right_side - apply_operator(
        padder(relaxed_potential), weights[level_index], level_scale
    )
    relaxed_potential = relaxed_potential + refine(
        vcycle(level_index + 1, coarsen(residual), None, weights, diagonals, padder, coarse_solve)
    )
    return (
        relaxed_potential
        + RELAXATION
        * (
            right_side
            - apply_operator(padder(relaxed_potential), weights[level_index], level_scale)
        )
        / diagonals[level_index]
    )


def call(body, outs, scratch=(), flops=1000, limit=16, name=None):
    single = isinstance(outs[0], int)
    shapes = [outs] if single else list(outs)
    out_shape = [jax.ShapeDtypeStruct(shape, jnp.float32) for shape in shapes]
    specs = [pl.BlockSpec(memory_space=pltpu.VMEM) for _ in shapes]

    def run(*args):
        return pl.pallas_call(
            body,
            out_shape=out_shape[0] if single else out_shape,
            in_specs=[pl.BlockSpec(memory_space=pltpu.VMEM) for _ in args],
            out_specs=specs[0] if single else specs,
            scratch_shapes=list(scratch),
            name=name,
            cost_estimate=pl.CostEstimate(flops=flops, transcendentals=0, bytes_accessed=1024),
            compiler_params=pltpu.CompilerParams(vmem_limit_bytes=limit << 20),
        )(*args)

    return run


def moved(value, tube_bits, lon_bits, tubes, lons):
    pairs = [
        (t * lons + l, (t ^ tube_bits) * lons + (l ^ lon_bits))
        for t in range(tubes)
        for l in range(lons)
    ]
    return lax.ppermute(value, ALL_AXES, pairs)


def cross_pairs(value, tubes, lons):
    pairs = []
    for t in range(tubes):
        for l in range(lons):
            other = (l + 1) % lons if l % 2 else (l - 1) % lons
            pairs.append((t * lons + l, t * lons + other))
    return lax.ppermute(value, ALL_AXES, pairs)


def tube_sums(pedersen_ref, wind_ref, out_ref):
    points = pedersen_ref.shape[0]
    first = [jnp.zeros(pedersen_ref.shape[1:], jnp.float32) for _ in range(4)]
    second = list(first)
    for p in range(points):
        conduct = pedersen_ref[p]
        first[p % 4] = first[p % 4] + conduct
        second[p % 4] = second[p % 4] + conduct * wind_ref[p]
    out_ref[0] = (first[0] + first[1]) + (first[2] + first[3])
    out_ref[1] = (second[0] + second[1]) + (second[2] + second[3])


def line_totals(density_ref, courant_ref, total_ref, keep_ref, gain_ref):
    species, points, lons, lats = density_ref.shape
    courant = jnp.broadcast_to(courant_ref[...][:, :, None], (species, points, lats))
    gain = 1.0 / (1.0 + courant)
    keep_ref[...] = courant * gain
    gain_ref[...] = gain
    retain = [jnp.ones((lons, lats), jnp.float32)] * species
    total = [jnp.zeros((lons, lats), jnp.float32)] * species
    for p in range(points):
        for s in range(species):
            keep = jnp.broadcast_to(keep_ref[s, pl.ds(p, 1), :], (lons, lats))
            give = jnp.broadcast_to(gain_ref[s, pl.ds(p, 1), :], (lons, lats))
            retain[s] = retain[s] * keep
            total[s] = keep * total[s] + give * density_ref[s, p]
    for s in range(species):
        total_ref[0, s] = retain[s]
        total_ref[1, s] = total[s]


def align_lines(density_ref, keep_ref, gain_ref, enter_ref, aligned_ref, core_ref, cross_ref):
    species, points, lons, lats = density_ref.shape
    odd = lax.rem(lax.axis_index("lon"), 2)
    state = [enter_ref[s] for s in range(species)]
    for p in range(points):
        for s in range(species):
            keep = jnp.broadcast_to(keep_ref[s, pl.ds(p, 1), :], (lons, lats))
            give = jnp.broadcast_to(gain_ref[s, pl.ds(p, 1), :], (lons, lats))
            state[s] = keep * state[s] + give * density_ref[s, p]
            aligned_ref[s, p] = state[s]
    rows = aligned_ref.reshape(species * points * lons, lats)
    near = jnp.where(odd == 1, 0, lons - 1)
    far = lons - 1 - near
    for s in range(species):
        base = s * points * lons
        core_ref[s] = rows[pl.ds(base + near, points, stride=lons), :]
        cross_ref[s] = rows[pl.ds(base + far, points, stride=lons), :]


def move_densities(aligned_ref, core_ref, cross_ref, coef_ref, out_ref):
    species, points, lons, lats = aligned_ref.shape
    centre, west, east, south, north, near, far = [coef_ref[i] for i in range(7)]
    for s in range(species):
        for p in range(points):
            here = aligned_ref[s, p]
            result = centre * here
            result = result + west * pltpu.roll(here, 1, 0) + east * pltpu.roll(here, lons - 1, 0)
            result = result + south * pltpu.roll(here, 1, 1) + north * pltpu.roll(here, lats - 1, 1)
            result = result + near * jnp.broadcast_to(core_ref[s, pl.ds(p, 1), :], (lons, lats))
            result = result + far * jnp.broadcast_to(cross_ref[s, pl.ds(p, 1), :], (lons, lats))
            out_ref[s, p] = result


ROWS = 8


def lane_of(lanes):
    return lax.broadcasted_iota(jnp.int32, (ROWS, lanes), 1)


def row_of(lanes):
    return lax.broadcasted_iota(jnp.int32, (ROWS, lanes), 0)


def row(value, index):
    return jnp.broadcast_to(value[index : index + 1, :], value.shape)


def lon_sides(fields):
    count = len(fields)
    west = [fields[k - 1] if k else pltpu.roll(fields[count - 1], 1, 0) for k in range(count)]
    east = [
        fields[k + 1] if k < count - 1 else pltpu.roll(fields[0], ROWS - 1, 0) for k in range(count)
    ]
    return west, east


def lat_sides(fields, step):
    lanes = fields[0].shape[1]
    return (
        [pltpu.roll(field, step, 1) for field in fields],
        [pltpu.roll(field, lanes - step, 1) for field in fields],
    )


def restricted(fields, level):
    lanes = fields[0].shape[1]
    step = 1 << level
    upper = (lane_of(lanes) & step) != 0
    out = []
    for k in range(0, len(fields), 2):
        pair = fields[k] + fields[k + 1]
        partner = jnp.where(upper, pltpu.roll(pair, step, 1), pltpu.roll(pair, lanes - step, 1))
        out.append(0.25 * (pair + partner))
    return out


class Level:
    def __init__(self, conduct, level):
        lanes = conduct[0].shape[1]
        self.step = 1 << level
        scale = 0.25**level
        lane = lane_of(lanes)
        first, last = lane < self.step, lane >= lanes - self.step
        west, east = lon_sides(conduct)
        south, north = lat_sides(conduct, self.step)
        self.west, self.east, self.south, self.north, self.own, self.diagonal = ([] for _ in range(6))
        for k, here in enumerate(conduct):
            half = (0.5 * scale) * here
            side_south = half + jnp.where(first, 0.0, (0.5 * scale) * south[k])
            side_north = half + jnp.where(last, 0.0, (0.5 * scale) * north[k])
            self.west.append(half + (0.5 * scale) * west[k])
            self.east.append(half + (0.5 * scale) * east[k])
            self.south.append(jnp.where(first, 0.0, side_south))
            self.north.append(jnp.where(last, 0.0, side_north))
            edge = jnp.where(first, side_south, 0.0) + jnp.where(last, side_north, 0.0)
            self.own.append(edge + SCREENING)
            self.diagonal.append(
                (self.west[k] + self.east[k]) + (side_south + side_north) + SCREENING
            )
        self.relax = [RELAXATION / value for value in self.diagonal]

    def apply(self, fields):
        west, east = lon_sides(fields)
        south, north = lat_sides(fields, self.step)
        return [
            (
                (self.own[k] * here + self.west[k] * (here - west[k]))
                + self.east[k] * (here - east[k])
            )
            + (self.south[k] * (here - south[k]) + self.north[k] * (here - north[k]))
            for k, here in enumerate(fields)
        ]


def small_inverse(columns):
    columns = list(columns)
    count = len(columns)
    rows = row_of(columns[0].shape[1])
    for p in range(count):
        pivot_column = columns[p]
        inverse = 1.0 / row(pivot_column, p)
        here = rows == p
        for j in range(count):
            if j != p:
                scaled = row(columns[j], p) * inverse
                columns[j] = jnp.where(here, scaled, columns[j] - pivot_column * scaled)
        columns[p] = jnp.where(here, inverse, -pivot_column * inverse)
    return columns


def times_vector(columns, vector):
    terms = [column * row(vector, a) for a, column in enumerate(columns)]
    while len(terms) > 1:
        terms = [terms[i] + terms[i + 1] for i in range(0, len(terms) - 1, 2)] + (
            [terms[-1]] if len(terms) % 2 else []
        )
    return terms[0]


def times_matrix(left, right):
    return [times_vector(left, column) for column in right]


class Coarse:
    def __init__(self, level, lanes):
        rows = row_of(lanes)
        west, east = level.west[0], level.east[0]
        low = [-level.south[0]]
        high = [-level.north[0]]
        self.first = level.step
        diagonal = []
        for a in range(ROWS):
            column = jnp.where(rows == a, level.diagonal[0], 0.0)
            column = jnp.where(rows == (a + 1) % ROWS, -west, column)
            diagonal.append(jnp.where(rows == (a - 1) % ROWS, -east, column))
        self.lanes = lanes
        self.steps = []
        step = level.step
        while step < lanes:
            inverse = small_inverse(diagonal)
            before = [pltpu.roll(column, step, 1) for column in inverse]
            after = [pltpu.roll(column, lanes - step, 1) for column in inverse]
            last = 2 * step >= lanes
            if len(low) == 1:
                down, up = low[0], high[0]
                alpha = [-down * column for column in before]
                gamma = [-up * column for column in after]
                diagonal = [
                    diagonal[c] + alpha[c] * row(down, c) + gamma[c] * row(up, c)
                    for c in range(ROWS)
                ]
                down_before = pltpu.roll(down, step, 1)
                up_after = pltpu.roll(up, lanes - step, 1)
                low = [alpha[c] * row(down_before, c) for c in range(ROWS)]
                high = [gamma[c] * row(up_after, c) for c in range(ROWS)]
            else:
                alpha = [-column for column in times_matrix(low, before)]
                gamma = [-column for column in times_matrix(high, after)]
                high_before = [pltpu.roll(column, step, 1) for column in high]
                low_after = [pltpu.roll(column, lanes - step, 1) for column in low]
                one, two = times_matrix(alpha, high_before), times_matrix(gamma, low_after)
                diagonal = [diagonal[c] + one[c] + two[c] for c in range(ROWS)]
                if not last:
                    low_before = [pltpu.roll(column, step, 1) for column in low]
                    high_after = [pltpu.roll(column, lanes - step, 1) for column in high]
                    low = times_matrix(alpha, low_before)
                    high = times_matrix(gamma, high_after)
            self.steps.append((step, alpha, gamma))
            step *= 2
        self.inverse = small_inverse(diagonal)

    def solve(self, right):
        for step, alpha, gamma in self.steps:
            before = pltpu.roll(right, step, 1)
            after = pltpu.roll(right, self.lanes - step, 1)
            right = right + times_vector(alpha, before) + times_vector(gamma, after)
        return times_vector(self.inverse, right)


def one_cycle(level_index, right, start, levels, coarse):
    if level_index == len(levels):
        return [coarse.solve(right[0])]
    level = levels[level_index]
    count = len(right)
    if start is None:
        value = [level.relax[k] * right[k] for k in range(count)]
    else:
        applied = level.apply(start)
        value = [start[k] + level.relax[k] * (right[k] - applied[k]) for k in range(count)]
    applied = level.apply(value)
    rest = [right[k] - applied[k] for k in range(count)]
    below = one_cycle(level_index + 1, restricted(rest, level_index), None, levels, coarse)
    value = [value[k] + below[k // 2] for k in range(count)]
    applied = level.apply(value)
    return [value[k] + level.relax[k] * (right[k] - applied[k]) for k in range(count)]


def stencil(here, lower, upper, odd):
    lanes = here.shape[1]
    lane, rows = lane_of(lanes), row_of(lanes)
    first, last = lane == 0, lane == lanes - 1
    west_sum, east_sum, across = lower + here, here + upper, upper - lower

    def slope(value):
        ahead = jnp.where(last, 0.0, pltpu.roll(value, lanes - 1, 1))
        behind = jnp.where(first, 0.0, pltpu.roll(value, 1, 1))
        return COURANT_CAP * jnp.tanh((-DRIFT_GAIN * 0.25) * (ahead - behind))

    lon_west, lon_east = slope(west_sum), slope(east_sum)
    lat_south = across + pltpu.roll(across, 1, 1)
    lat_north = across + pltpu.roll(across, lanes - 1, 1)
    lat_south = jnp.where(first, 0.0, COURANT_CAP * jnp.tanh((DRIFT_GAIN * 0.25) * lat_south))
    lat_north = jnp.where(last, 0.0, COURANT_CAP * jnp.tanh((DRIFT_GAIN * 0.25) * lat_north))
    out_east, in_east = jnp.maximum(lon_east, 0.0), jnp.minimum(lon_east, 0.0)
    in_west, out_west = jnp.maximum(lon_west, 0.0), jnp.minimum(lon_west, 0.0)
    out_north, in_north = jnp.maximum(lat_north, 0.0), jnp.minimum(lat_north, 0.0)
    in_south, out_south = jnp.maximum(lat_south, 0.0), jnp.minimum(lat_south, 0.0)
    centre = 1.0 - (out_east - out_west) - (out_north - out_south)
    west, east = in_west, -in_east
    top, bottom = rows == 0, rows == ROWS - 1
    from_west = jnp.where(top, west, 0.0)
    from_east = jnp.where(bottom, east, 0.0)
    near = jnp.where(odd == 1, from_west, from_east)
    far = jnp.where(odd == 1, from_east, from_west)
    return (
        centre,
        jnp.where(top, 0.0, west),
        jnp.where(bottom, 0.0, east),
        in_south,
        -in_north,
        near,
        far,
    )


def solve_potential(shares, points, held, *refs):
    pieces, (coef_ref, potential_ref, scratch) = refs[:-3], refs[-3:]
    here = lax.axis_index("lon")
    at = 0
    lats = scratch.shape[2]
    lons = scratch.shape[1]
    for piece in pieces:
        for slot in range(piece.shape[0]):
            block = jnp.bitwise_xor(here, held[at])
            at += 1
            for field in range(2):
                scratch[field, pl.ds(pl.multiple_of(block * ROWS, ROWS), ROWS), :] = piece[slot, field]
    count = lons // ROWS
    conduct = [(1.0 / points) * scratch[0, pl.ds(k, ROWS, stride=count), :] for k in range(count)]
    source = [(1.0 / points) * scratch[1, pl.ds(k, ROWS, stride=count), :] for k in range(count)]
    levels = []
    for index in range(LEVELS):
        levels.append(Level(conduct, index))
        conduct = restricted(conduct, index)
    coarse = Coarse(Level(conduct, LEVELS), lats)
    value = None
    for _ in range(CYCLES):
        value = one_cycle(0, source, value, levels, coarse)
    for k in range(count):
        scratch[0, pl.ds(k, ROWS, stride=count), :] = value[k]
    start = here * ROWS
    own = scratch[0, pl.ds(pl.multiple_of(start, ROWS), ROWS), :]
    rows = row_of(lats)
    left = scratch[0, pl.ds(lax.rem(start + lons - 1, lons), 1), :]
    right = scratch[0, pl.ds(lax.rem(start + ROWS, lons), 1), :]
    lower = jnp.where(rows == 0, jnp.broadcast_to(left, own.shape), pltpu.roll(own, 1, 0))
    upper = jnp.where(
        rows == ROWS - 1, jnp.broadcast_to(right, own.shape), pltpu.roll(own, ROWS - 1, 0)
    )
    potential_ref[...] = own
    for i, value in enumerate(stencil(own, lower, upper, lax.rem(here, 2))):
        coef_ref[i] = value


def plain_potential(conductance, source, own_lons):
    conductances = [conductance]
    for level_index in range(LEVELS):
        conductances.append(coarsen(conductances[-1]))
    weights = [face_weights(grid_pad(conductances[level_index])) for level_index in range(LEVELS)]
    diagonals = [
        diagonal_of(weights[level_index], 0.25**level_index) for level_index in range(LEVELS)
    ]
    factor = jnp.linalg.cholesky(dense_operator(conductances[LEVELS], 0.25**LEVELS))

    def coarse_solve(right_side):
        return jax.scipy.linalg.cho_solve((factor, True), right_side.reshape(-1)).reshape(
            right_side.shape
        )

    potential = None
    for _ in range(CYCLES):
        potential = vcycle(0, source, potential, weights, diagonals, grid_pad, coarse_solve)
    here = lax.axis_index("lon")
    around = jnp.concatenate([potential[-1:], potential, potential[:1]], axis=0)
    window = lax.dynamic_slice(
        around, (here * own_lons, jnp.zeros((), jnp.int32)), (own_lons + 2, potential.shape[1])
    )

    def body(window_ref, coef_ref):
        own = window_ref[1 : own_lons + 1]
        odd = lax.rem(lax.axis_index("lon"), 2)
        parts = stencil(own, window_ref[0:own_lons], window_ref[2 : own_lons + 2], odd)
        for i, value in enumerate(parts):
            coef_ref[i] = value

    coefs = call(body, (7, own_lons, potential.shape[1]), name="coefs")(window)
    return coefs, window[1 : own_lons + 1]


def on_device(density, pedersen, neutral_wind, along_courant):
    tubes, lons = lax.axis_size("tube"), lax.axis_size("lon")
    species, points, own_lons, lats = density.shape
    whole_lons = own_lons * lons
    line_points = points * tubes
    block = (own_lons, lats)
    tube_here = lax.axis_index("tube")

    part = call(tube_sums, (2, *block), flops=2000, name="tube_sums")(pedersen, neutral_wind)
    other = moved(part, 0, 1, tubes, lons)
    summary, keep, gain = call(
        line_totals,
        [(2, species, *block), (species, points, lats), (species, points, lats)],
        flops=2000000,
        name="line_totals",
    )(density, along_courant)
    stack = jnp.stack([part, other])
    group_keep, group_total = summary[0], summary[1]
    enter = jnp.zeros((species, *block), jnp.float32)
    enter_keep = jnp.ones((species, *block), jnp.float32)
    bit = 1
    while bit < tubes:
        received = moved(stack, bit, 1, tubes, lons)
        sent = jnp.stack([group_keep, group_total])
        theirs = moved(sent, bit, 0, tubes, lons)
        stack = stack + received[::-1]
        is_upper = (tube_here & bit) != 0
        enter = jnp.where(is_upper, enter_keep * theirs[1] + enter, enter)
        enter_keep = jnp.where(is_upper, enter_keep * theirs[0], enter_keep)
        early_total = jnp.where(is_upper, theirs[1], group_total)
        late_total = jnp.where(is_upper, group_total, theirs[1])
        late_keep = jnp.where(is_upper, group_keep, theirs[0])
        group_total = late_keep * early_total + late_total
        group_keep = group_keep * theirs[0]
        bit *= 2
    aligned, to_core, to_cross = call(
        align_lines,
        [density.shape, (species, points, lats), (species, points, lats)],
        flops=2000000,
        name="align_lines",
    )(density, keep, gain, enter)
    held = [0, 1]
    pieces = [stack]
    bit = 2
    while bit < lons:
        if len(pieces) > 1:
            pieces = [jnp.concatenate(pieces)]
        pieces.append(moved(pieces[0], 0, bit ^ 1, tubes, lons))
        held = held + [bit ^ 1 ^ offset for offset in held]
        bit *= 2
    from_core = moved(to_core, 0, 1, tubes, lons)
    from_cross = cross_pairs(to_cross, tubes, lons)
    if whole_lons >> LEVELS == ROWS and own_lons == ROWS:
        coefs, potential = call(
            functools.partial(solve_potential, None, line_points, held),
            [(7, *block), block],
            scratch=[pltpu.VMEM((2, whole_lons, lats), jnp.float32)],
            flops=20000000,
            name="solve_potential",
        )(*pieces)
    else:
        slots = jnp.concatenate(pieces)
        order = jnp.bitwise_xor(jnp.arange(lons), lax.axis_index("lon"))
        where_held = [0] * lons
        for at, offset in enumerate(held):
            where_held[offset] = at
        blocks = jnp.take(slots, jnp.take(jnp.array(where_held), order), axis=0)
        grids = jnp.moveaxis(blocks, 1, 0).reshape(2, whole_lons, lats) / line_points
        coefs, potential = plain_potential(grids[0], grids[1], own_lons)
    density_next = call(move_densities, density.shape, flops=4000000, name="move_densities")(
        aligned, from_core, from_cross, coefs
    )
    return (density_next, potential)


def solution(mesh):
    return jax.shard_map(
        on_device,
        mesh=mesh,
        in_specs=(
            P(None, "tube", "lon", None),
            P("tube", "lon", None),
            P("tube", "lon", None),
            P(None, "tube"),
        ),
        out_specs=(P(None, "tube", "lon", None), P("lon", None)),
        check_vma=False,
    )
```

```python
import functools

import jax
import jax.numpy as jnp
from jax import lax
from jax.experimental import pallas as pl
from jax.experimental.pallas import tpu as pltpu
from jax.sharding import PartitionSpec as P

LEVELS = 3
CYCLES = 3


SCREENING = 0.005
RELAXATION = 0.8
DRIFT_GAIN = 1.0
COURANT_CAP = 0.2
ALL_AXES = ("tube", "lon")


def lat_zeros(periodic_copy):
    return jnp.pad(periodic_copy, ((0, 0), (1, 1)))


def grid_pad(grid_field):
    periodic_copy = jnp.concatenate([grid_field[-1:], grid_field, grid_field[:1]], axis=0)
    return lat_zeros(periodic_copy)


def face_weights(cond_pad):
    middle = cond_pad[1:-1, 1:-1]
    return (
        0.5 * (cond_pad[:-2, 1:-1] + middle),
        0.5 * (cond_pad[2:, 1:-1] + middle),
        0.5 * (cond_pad[1:-1, :-2] + middle),
        0.5 * (cond_pad[1:-1, 2:] + middle),
    )


def apply_operator(field_pad, weights, level_scale):
    middle = field_pad[1:-1, 1:-1]
    net_flux = weights[0] * (middle - field_pad[:-2, 1:-1]) + weights[1] * (
        middle - field_pad[2:, 1:-1]
    )
    net_flux = (
        net_flux
        + weights[2] * (middle - field_pad[1:-1, :-2])
        + weights[3] * (middle - field_pad[1:-1, 2:])
    )
    return level_scale * net_flux + SCREENING * middle


def diagonal_of(weights, level_scale):
    return level_scale * (weights[0] + weights[1] + weights[2] + weights[3]) + SCREENING


def coarsen(grid_field):
    return 0.25 * grid_field.reshape(grid_field.shape[0] // 2, 2, grid_field.shape[1] // 2, 2).sum(
        axis=(1, 3)
    )


def refine(grid_field):
    return jnp.repeat(jnp.repeat(grid_field, 2, axis=0), 2, axis=1)


def dense_operator(grid_cond, level_scale):
    unknowns = grid_cond.shape[0] * grid_cond.shape[1]
    weights = face_weights(grid_pad(grid_cond))
    unit_fields = jnp.eye(unknowns, dtype=jnp.float32).reshape(
        unknowns, grid_cond.shape[0], grid_cond.shape[1]
    )
    matrix_rows = jax.vmap(
        lambda unit_field: apply_operator(grid_pad(unit_field), weights, level_scale)
    )(unit_fields)
    return matrix_rows.reshape(unknowns, unknowns)


def vcycle(level_index, right_side, start_field, weights, diagonals, padder, coarse_solve):
    if level_index == len(weights):
        return coarse_solve(right_side)
    level_scale = 0.25**level_index
    if start_field is None:
        relaxed_potential = RELAXATION * right_side / diagonals[level_index]
    else:
        relaxed_potential = (
            start_field
            + RELAXATION
            * (right_side - apply_operator(padder(start_field), weights[level_index], level_scale))
            / diagonals[level_index]
        )
    residual = right_side - apply_operator(
        padder(relaxed_potential), weights[level_index], level_scale
    )
    relaxed_potential = relaxed_potential + refine(
        vcycle(level_index + 1, coarsen(residual), None, weights, diagonals, padder, coarse_solve)
    )
    return (
        relaxed_potential
        + RELAXATION
        * (
            right_side
            - apply_operator(padder(relaxed_potential), weights[level_index], level_scale)
        )
        / diagonals[level_index]
    )


def call(body, outs, scratch=(), flops=1000, limit=16, name=None, ins=None, places=None):
    single = isinstance(outs[0], int)
    shapes = [outs] if single else list(outs)
    out_shape = [jax.ShapeDtypeStruct(shape, jnp.float32) for shape in shapes]
    places = places or [pltpu.VMEM] * len(shapes)
    specs = [pl.BlockSpec(memory_space=place) for place in places]

    def run(*args):
        given = ins or [pltpu.VMEM] * len(args)
        args = [
            pltpu.with_memory_space_constraint(arg, place) if place is pltpu.HBM else arg
            for arg, place in zip(args, given)
        ]
        return pl.pallas_call(
            body,
            out_shape=out_shape[0] if single else out_shape,
            in_specs=[pl.BlockSpec(memory_space=place) for place in given],
            out_specs=specs[0] if single else specs,
            scratch_shapes=list(scratch),
            name=name,
            cost_estimate=pl.CostEstimate(flops=flops, transcendentals=0, bytes_accessed=1024),
            compiler_params=pltpu.CompilerParams(vmem_limit_bytes=int(limit * 2**20)),
        )(*args)

    return run


def moved(value, tube_bits, lon_bits, tubes, lons):
    pairs = [
        (t * lons + l, (t ^ tube_bits) * lons + (l ^ lon_bits))
        for t in range(tubes)
        for l in range(lons)
    ]
    return lax.ppermute(value, ALL_AXES, pairs)


def cross_pairs(value, tubes, lons):
    pairs = []
    for t in range(tubes):
        for l in range(lons):
            other = (l + 1) % lons if l % 2 else (l - 1) % lons
            pairs.append((t * lons + l, t * lons + other))
    return lax.ppermute(value, ALL_AXES, pairs)


def tube_sums(
    pedersen_hbm,
    wind_hbm,
    density_hbm,
    courant_hbm,
    out_ref,
    density_ref,
    keep_ref,
    gain_ref,
    pedersen_ref,
    wind_ref,
    courant_ref,
    sems,
):
    species, points, _, lats = density_ref.shape
    copies = [
        pltpu.make_async_copy(pedersen_hbm, pedersen_ref, sems.at[0]),
        pltpu.make_async_copy(wind_hbm, wind_ref, sems.at[1]),
        pltpu.make_async_copy(courant_hbm, courant_ref, sems.at[2]),
        pltpu.make_async_copy(density_hbm, density_ref, sems.at[3]),
    ]
    for copy in copies:
        copy.start()
    copies[2].wait()
    courant = jnp.broadcast_to(courant_ref[...][:, :, None], (species, points, lats))
    gain = 1.0 / (1.0 + courant)
    keep_ref[...] = courant * gain
    gain_ref[...] = gain
    copies[0].wait()
    copies[1].wait()
    first = [jnp.zeros(pedersen_ref.shape[1:], jnp.float32) for _ in range(4)]
    second = list(first)
    for p in range(points):
        conduct = pedersen_ref[p]
        first[p % 4] = first[p % 4] + conduct
        second[p % 4] = second[p % 4] + conduct * wind_ref[p]
    out_ref[0] = (first[0] + first[1]) + (first[2] + first[3])
    out_ref[1] = (second[0] + second[1]) + (second[2] + second[3])
    copies[3].wait()


def line_totals(density_ref, keep_ref, gain_ref, out_ref):
    species, points, lons, lats = density_ref.shape
    flat = keep_ref.reshape(species * points, lats)
    retain = jnp.ones((species, lats), jnp.float32)
    total = [jnp.zeros((lons, lats), jnp.float32)] * species
    for p in range(points):
        retain = retain * flat[pl.ds(p, species, stride=points), :]
        for s in range(species):
            keep = jnp.broadcast_to(keep_ref[s, pl.ds(p, 1), :], (lons, lats))
            give = jnp.broadcast_to(gain_ref[s, pl.ds(p, 1), :], (lons, lats))
            total[s] = keep * total[s] + give * density_ref[s, p]
    for s in range(species):
        out_ref[s] = total[s]
        out_ref[species, s : s + 1, :] = retain[s : s + 1, :]
    for s in range(species, lons):
        out_ref[species, s : s + 1, :] = jnp.zeros((1, lats), jnp.float32)


def first_message(own_ref, other_ref, lines_ref, out_ref):
    for field in range(2):
        out_ref[field] = own_ref[field]
        out_ref[2 + field] = other_ref[field]
    out_ref[4:] = lines_ref[...]


def join_lines(bit, last, mine_ref, theirs_ref, enter_ref, out_ref, next_ref):
    species = enter_ref.shape[0] - 1
    upper = jnp.bitwise_and(lax.axis_index("tube"), bit) != 0
    shape = mine_ref.shape[1:]
    above = jnp.broadcast_to(upper, shape)
    for i in range(4):
        out_ref[i] = mine_ref[i] + theirs_ref[i]
    mine_keep, theirs_keep = mine_ref[4 + species], theirs_ref[4 + species]
    enter_keep = enter_ref[species]
    next_ref[species] = jnp.where(above, enter_keep * theirs_keep, enter_keep)
    late_keep = jnp.where(above, mine_keep, theirs_keep)
    for s in range(species):
        theirs, enter = theirs_ref[4 + s], enter_ref[s]
        next_ref[s] = jnp.where(above, row(enter_keep, s) * theirs + enter, enter)
        if not last:
            mine = mine_ref[4 + s]
            early = jnp.where(above, theirs, mine)
            late = jnp.where(above, mine, theirs)
            out_ref[4 + s] = row(late_keep, s) * early + late
    if not last:
        out_ref[4 + species] = mine_keep * theirs_keep


def align_lines(density_ref, keep_ref, gain_ref, enter_ref, aligned_ref, core_ref, cross_ref):
    species, points, lons, lats = density_ref.shape
    odd = lax.rem(lax.axis_index("lon"), 2)
    state = [enter_ref[s] for s in range(species)]
    for p in range(points):
        for s in range(species):
            keep = jnp.broadcast_to(keep_ref[s, pl.ds(p, 1), :], (lons, lats))
            give = jnp.broadcast_to(gain_ref[s, pl.ds(p, 1), :], (lons, lats))
            state[s] = keep * state[s] + give * density_ref[s, p]
            aligned_ref[s, p] = state[s]
    rows = aligned_ref.reshape(species * points * lons, lats)
    near = jnp.where(odd == 1, 0, lons - 1)
    far = lons - 1 - near
    for s in range(species):
        base = s * points * lons
        core_ref[s] = rows[pl.ds(base + near, points, stride=lons), :]
        cross_ref[s] = rows[pl.ds(base + far, points, stride=lons), :]


def move_densities(aligned_ref, core_ref, cross_ref, coef_ref, out_hbm, potential_hbm, out_ref, sems):
    species, points, lons, lats = aligned_ref.shape
    field_copy = pltpu.make_async_copy(coef_ref.at[7], potential_hbm, sems.at[species])
    field_copy.start()
    centre, west, east, south, north, near, far = [coef_ref[i] for i in range(7)]
    copies = []
    for s in range(species):
        for p in range(points):
            here = aligned_ref[s, p]
            result = centre * here
            result = result + west * pltpu.roll(here, 1, 0) + east * pltpu.roll(here, lons - 1, 0)
            result = result + south * pltpu.roll(here, 1, 1) + north * pltpu.roll(here, lats - 1, 1)
            result = result + near * jnp.broadcast_to(core_ref[s, pl.ds(p, 1), :], (lons, lats))
            result = result + far * jnp.broadcast_to(cross_ref[s, pl.ds(p, 1), :], (lons, lats))
            out_ref[s, p] = result
        copies.append(pltpu.make_async_copy(out_ref.at[s], out_hbm.at[s], sems.at[s]))
        copies[-1].start()
    field_copy.wait()
    for copy in copies:
        copy.wait()


ROWS = 8


def lane_of(lanes):
    return lax.broadcasted_iota(jnp.int32, (ROWS, lanes), 1)


def row_of(lanes):
    return lax.broadcasted_iota(jnp.int32, (ROWS, lanes), 0)


def row(value, index):
    return jnp.broadcast_to(value[index : index + 1, :], value.shape)


def lon_sides(fields):
    count = len(fields)
    west = [fields[k - 1] if k else pltpu.roll(fields[count - 1], 1, 0) for k in range(count)]
    east = [
        fields[k + 1] if k < count - 1 else pltpu.roll(fields[0], ROWS - 1, 0) for k in range(count)
    ]
    return west, east


def lat_sides(fields, step):
    lanes = fields[0].shape[1]
    return (
        [pltpu.roll(field, step, 1) for field in fields],
        [pltpu.roll(field, lanes - step, 1) for field in fields],
    )


def restricted(fields, level):
    lanes = fields[0].shape[1]
    step = 1 << level
    upper = (lane_of(lanes) & step) != 0
    out = []
    for k in range(0, len(fields), 2):
        pair = fields[k] + fields[k + 1]
        partner = jnp.where(upper, pltpu.roll(pair, step, 1), pltpu.roll(pair, lanes - step, 1))
        out.append(0.25 * (pair + partner))
    return out


class Level:
    def __init__(self, conduct, level):
        lanes = conduct[0].shape[1]
        self.step = 1 << level
        scale = 0.25**level
        lane = lane_of(lanes)
        first, last = lane < self.step, lane >= lanes - self.step
        west, east = lon_sides(conduct)
        south, north = lat_sides(conduct, self.step)
        self.west, self.east, self.south, self.north, self.own, self.diagonal = ([] for _ in range(6))
        for k, here in enumerate(conduct):
            half = (0.5 * scale) * here
            side_south = half + jnp.where(first, 0.0, (0.5 * scale) * south[k])
            side_north = half + jnp.where(last, 0.0, (0.5 * scale) * north[k])
            self.west.append(half + (0.5 * scale) * west[k])
            self.east.append(half + (0.5 * scale) * east[k])
            self.south.append(jnp.where(first, 0.0, side_south))
            self.north.append(jnp.where(last, 0.0, side_north))
            edge = jnp.where(first, side_south, 0.0) + jnp.where(last, side_north, 0.0)
            self.own.append(edge + SCREENING)
            self.diagonal.append(
                (self.west[k] + self.east[k]) + (side_south + side_north) + SCREENING
            )
        self.relax = [RELAXATION / value for value in self.diagonal]

    def apply(self, fields):
        west, east = lon_sides(fields)
        south, north = lat_sides(fields, self.step)
        return [
            (
                (self.own[k] * here + self.west[k] * (here - west[k]))
                + self.east[k] * (here - east[k])
            )
            + (self.south[k] * (here - south[k]) + self.north[k] * (here - north[k]))
            for k, here in enumerate(fields)
        ]


def small_inverse(columns):
    columns = list(columns)
    count = len(columns)
    rows = row_of(columns[0].shape[1])
    for p in range(count):
        pivot_column = columns[p]
        inverse = 1.0 / row(pivot_column, p)
        here = rows == p
        for j in range(count):
            if j != p:
                scaled = row(columns[j], p) * inverse
                columns[j] = jnp.where(here, scaled, columns[j] - pivot_column * scaled)
        columns[p] = jnp.where(here, inverse, -pivot_column * inverse)
    return columns


def times_vector(columns, vector):
    terms = [column * row(vector, a) for a, column in enumerate(columns)]
    while len(terms) > 1:
        terms = [terms[i] + terms[i + 1] for i in range(0, len(terms) - 1, 2)] + (
            [terms[-1]] if len(terms) % 2 else []
        )
    return terms[0]


def times_matrix(left, right):
    return [times_vector(left, column) for column in right]


class Coarse:
    def __init__(self, level, lanes):
        rows = row_of(lanes)
        west, east = level.west[0], level.east[0]
        low = [-level.south[0]]
        high = [-level.north[0]]
        self.first = level.step
        diagonal = []
        for a in range(ROWS):
            column = jnp.where(rows == a, level.diagonal[0], 0.0)
            column = jnp.where(rows == (a + 1) % ROWS, -west, column)
            diagonal.append(jnp.where(rows == (a - 1) % ROWS, -east, column))
        self.lanes = lanes
        self.steps = []
        step = level.step
        while step < lanes:
            inverse = small_inverse(diagonal)
            before = [pltpu.roll(column, step, 1) for column in inverse]
            after = [pltpu.roll(column, lanes - step, 1) for column in inverse]
            last = 2 * step >= lanes
            if len(low) == 1:
                down, up = low[0], high[0]
                alpha = [-down * column for column in before]
                gamma = [-up * column for column in after]
                diagonal = [
                    diagonal[c] + alpha[c] * row(down, c) + gamma[c] * row(up, c)
                    for c in range(ROWS)
                ]
                down_before = pltpu.roll(down, step, 1)
                up_after = pltpu.roll(up, lanes - step, 1)
                low = [alpha[c] * row(down_before, c) for c in range(ROWS)]
                high = [gamma[c] * row(up_after, c) for c in range(ROWS)]
            else:
                alpha = [-column for column in times_matrix(low, before)]
                gamma = [-column for column in times_matrix(high, after)]
                high_before = [pltpu.roll(column, step, 1) for column in high]
                low_after = [pltpu.roll(column, lanes - step, 1) for column in low]
                one, two = times_matrix(alpha, high_before), times_matrix(gamma, low_after)
                diagonal = [diagonal[c] + one[c] + two[c] for c in range(ROWS)]
                if not last:
                    low_before = [pltpu.roll(column, step, 1) for column in low]
                    high_after = [pltpu.roll(column, lanes - step, 1) for column in high]
                    low = times_matrix(alpha, low_before)
                    high = times_matrix(gamma, high_after)
            self.steps.append((step, alpha, gamma))
            step *= 2
        self.inverse = small_inverse(diagonal)

    def solve(self, right):
        for step, alpha, gamma in self.steps:
            before = pltpu.roll(right, step, 1)
            after = pltpu.roll(right, self.lanes - step, 1)
            right = right + times_vector(alpha, before) + times_vector(gamma, after)
        return times_vector(self.inverse, right)


def one_cycle(level_index, right, start, levels, coarse):
    if level_index == len(levels):
        return [coarse.solve(right[0])]
    level = levels[level_index]
    count = len(right)
    if start is None:
        value = [level.relax[k] * right[k] for k in range(count)]
    else:
        applied = level.apply(start)
        value = [start[k] + level.relax[k] * (right[k] - applied[k]) for k in range(count)]
    applied = level.apply(value)
    rest = [right[k] - applied[k] for k in range(count)]
    below = one_cycle(level_index + 1, restricted(rest, level_index), None, levels, coarse)
    value = [value[k] + below[k // 2] for k in range(count)]
    applied = level.apply(value)
    return [value[k] + level.relax[k] * (right[k] - applied[k]) for k in range(count)]


def stencil(here, lower, upper, odd):
    lanes = here.shape[1]
    lane, rows = lane_of(lanes), row_of(lanes)
    first, last = lane == 0, lane == lanes - 1
    west_sum, east_sum, across = lower + here, here + upper, upper - lower

    def slope(value):
        ahead = jnp.where(last, 0.0, pltpu.roll(value, lanes - 1, 1))
        behind = jnp.where(first, 0.0, pltpu.roll(value, 1, 1))
        return COURANT_CAP * jnp.tanh((-DRIFT_GAIN * 0.25) * (ahead - behind))

    lon_west, lon_east = slope(west_sum), slope(east_sum)
    lat_south = across + pltpu.roll(across, 1, 1)
    lat_north = across + pltpu.roll(across, lanes - 1, 1)
    lat_south = jnp.where(first, 0.0, COURANT_CAP * jnp.tanh((DRIFT_GAIN * 0.25) * lat_south))
    lat_north = jnp.where(last, 0.0, COURANT_CAP * jnp.tanh((DRIFT_GAIN * 0.25) * lat_north))
    out_east, in_east = jnp.maximum(lon_east, 0.0), jnp.minimum(lon_east, 0.0)
    in_west, out_west = jnp.maximum(lon_west, 0.0), jnp.minimum(lon_west, 0.0)
    out_north, in_north = jnp.maximum(lat_north, 0.0), jnp.minimum(lat_north, 0.0)
    in_south, out_south = jnp.maximum(lat_south, 0.0), jnp.minimum(lat_south, 0.0)
    centre = 1.0 - (out_east - out_west) - (out_north - out_south)
    west, east = in_west, -in_east
    top, bottom = rows == 0, rows == ROWS - 1
    from_west = jnp.where(top, west, 0.0)
    from_east = jnp.where(bottom, east, 0.0)
    near = jnp.where(odd == 1, from_west, from_east)
    far = jnp.where(odd == 1, from_east, from_west)
    return (
        centre,
        jnp.where(top, 0.0, west),
        jnp.where(bottom, 0.0, east),
        in_south,
        -in_north,
        near,
        far,
    )


def solve_potential(points, held, *refs):
    pieces, (coef_ref, scratch) = refs[:-2], refs[-2:]
    here = lax.axis_index("lon")
    at = 0
    lats = scratch.shape[2]
    lons = scratch.shape[1]
    for piece in pieces:
        for slot in range(piece.shape[0]):
            block = jnp.bitwise_xor(here, held[at])
            at += 1
            for field in range(2):
                scratch[field, pl.ds(pl.multiple_of(block * ROWS, ROWS), ROWS), :] = piece[slot, field]
    count = lons // ROWS
    conduct = [(1.0 / points) * scratch[0, pl.ds(k, ROWS, stride=count), :] for k in range(count)]
    source = [(1.0 / points) * scratch[1, pl.ds(k, ROWS, stride=count), :] for k in range(count)]
    levels = []
    for index in range(LEVELS):
        levels.append(Level(conduct, index))
        conduct = restricted(conduct, index)
    coarse = Coarse(Level(conduct, LEVELS), lats)
    value = None
    for _ in range(CYCLES):
        value = one_cycle(0, source, value, levels, coarse)
    for k in range(count):
        scratch[0, pl.ds(k, ROWS, stride=count), :] = value[k]
    start = here * ROWS
    own = scratch[0, pl.ds(pl.multiple_of(start, ROWS), ROWS), :]
    rows = row_of(lats)
    left = scratch[0, pl.ds(lax.rem(start + lons - 1, lons), 1), :]
    right = scratch[0, pl.ds(lax.rem(start + ROWS, lons), 1), :]
    lower = jnp.where(rows == 0, jnp.broadcast_to(left, own.shape), pltpu.roll(own, 1, 0))
    upper = jnp.where(
        rows == ROWS - 1, jnp.broadcast_to(right, own.shape), pltpu.roll(own, ROWS - 1, 0)
    )
    coef_ref[7] = own
    for i, value in enumerate(stencil(own, lower, upper, lax.rem(here, 2))):
        coef_ref[i] = value


def plain_potential(conductance, source, own_lons):
    conductances = [conductance]
    for level_index in range(LEVELS):
        conductances.append(coarsen(conductances[-1]))
    weights = [face_weights(grid_pad(conductances[level_index])) for level_index in range(LEVELS)]
    diagonals = [
        diagonal_of(weights[level_index], 0.25**level_index) for level_index in range(LEVELS)
    ]
    factor = jnp.linalg.cholesky(dense_operator(conductances[LEVELS], 0.25**LEVELS))

    def coarse_solve(right_side):
        return jax.scipy.linalg.cho_solve((factor, True), right_side.reshape(-1)).reshape(
            right_side.shape
        )

    potential = None
    for _ in range(CYCLES):
        potential = vcycle(0, source, potential, weights, diagonals, grid_pad, coarse_solve)
    here = lax.axis_index("lon")
    around = jnp.concatenate([potential[-1:], potential, potential[:1]], axis=0)
    window = lax.dynamic_slice(
        around, (here * own_lons, jnp.zeros((), jnp.int32)), (own_lons + 2, potential.shape[1])
    )

    def body(window_ref, coef_ref):
        own = window_ref[1 : own_lons + 1]
        odd = lax.rem(lax.axis_index("lon"), 2)
        parts = stencil(own, window_ref[0:own_lons], window_ref[2 : own_lons + 2], odd)
        for i, value in enumerate(parts):
            coef_ref[i] = value

        coef_ref[7] = own

    return call(body, (8, own_lons, potential.shape[1]), name="coefs")(window)


def on_device(density, pedersen, neutral_wind, along_courant):
    tubes, lons = lax.axis_size("tube"), lax.axis_size("lon")
    species, points, own_lons, lats = density.shape
    whole_lons = own_lons * lons
    line_points = points * tubes
    block = (own_lons, lats)
    near_line = (species, points, lats)

    part, local, keep, gain = call(
        tube_sums,
        [(2, *block), density.shape, near_line, near_line],
        scratch=[
            pltpu.VMEM(pedersen.shape, jnp.float32),
            pltpu.VMEM(pedersen.shape, jnp.float32),
            pltpu.VMEM(along_courant.shape, jnp.float32),
            pltpu.SemaphoreType.DMA((4,)),
        ],
        flops=2000,
        name="tube_sums",
        ins=[pltpu.HBM] * 4,
    )(pedersen, neutral_wind, density, along_courant)
    other = moved(part, 0, 1, tubes, lons)
    lines = call(line_totals, (species + 1, *block), flops=2000000, name="line_totals")(
        local, keep, gain
    )
    stack = call(first_message, (species + 5, *block), name="first_message")(part, other, lines)
    enter = jnp.concatenate(
        [jnp.zeros((species, *block), jnp.float32), jnp.ones((1, *block), jnp.float32)]
    )
    bit = 1
    while bit < tubes:
        last = 2 * bit >= tubes
        received = moved(stack, bit, 0, tubes, lons)
        stack, enter = call(
            functools.partial(join_lines, bit, last),
            [(4 if last else species + 5, *block), enter.shape],
            name="join_lines",
        )(stack, received, enter)
        bit *= 2
    stack = stack[:4].reshape(2, 2, *block)
    aligned, to_core, to_cross = call(
        align_lines, [density.shape, near_line, near_line], flops=2000000, name="align_lines"
    )(local, keep, gain, enter)
    held = [0, 1]
    pieces = [stack]
    bit = 2
    while bit < lons:
        if len(pieces) > 1:
            pieces = [jnp.concatenate(pieces)]
        pieces.append(moved(pieces[0], 0, bit ^ 1, tubes, lons))
        held = held + [bit ^ 1 ^ offset for offset in held]
        bit *= 2
    from_core = moved(to_core, 0, 1, tubes, lons)
    from_cross = cross_pairs(to_cross, tubes, lons)
    if whole_lons >> LEVELS == ROWS and own_lons == ROWS:
        coefs = call(
            functools.partial(solve_potential, line_points, held),
            (8, *block),
            scratch=[pltpu.VMEM((2, whole_lons, lats), jnp.float32)],
            flops=20000000,
            name="solve_potential",
        )(*pieces)
    else:
        slots = jnp.concatenate(pieces)
        order = jnp.bitwise_xor(jnp.arange(lons), lax.axis_index("lon"))
        where_held = [0] * lons
        for at, offset in enumerate(held):
            where_held[offset] = at
        blocks = jnp.take(slots, jnp.take(jnp.array(where_held), order), axis=0)
        grids = jnp.moveaxis(blocks, 1, 0).reshape(2, whole_lons, lats) / line_points
        coefs = plain_potential(grids[0], grids[1], own_lons)
    density_next, potential = call(
        move_densities,
        [density.shape, block],
        scratch=[
            pltpu.VMEM(density.shape, jnp.float32),
            pltpu.SemaphoreType.DMA((species + 1,)),
        ],
        flops=4000000,
        name="move_densities",
        places=[pltpu.HBM] * 2,
    )(aligned, from_core, from_cross, coefs)
    return (density_next, potential)


def solution(mesh):
    return jax.shard_map(
        on_device,
        mesh=mesh,
        in_specs=(
            P(None, "tube", "lon", None),
            P("tube", "lon", None),
            P("tube", "lon", None),
            P(None, "tube"),
        ),
        out_specs=(P(None, "tube", "lon", None), P("lon", None)),
        check_vma=False,
    )
```
